8 devices in a mesh: dp: 1 (over z), tp: 8 (over x, y, core).
Axes of the slice: x: 2, y: 2, z: 1, core: 2. Of those that a mesh axis runs over, the one named last changes fastest.
Arguments:
- x: bfloat16 [2048, 7168], P('dp')
- w_gate: bfloat16 [7168, 20480], P(None, 'tp')
- w_up: bfloat16 [7168, 20480], P(None, 'tp')
- w_down: bfloat16 [20480, 7168], P('tp')
Outputs:
- output: bfloat16 [2048, 7168], P('dp')
All inputs are finite; a program needn't handle non-finite values.
Results may differ from the reference program's by a relative error of at most 0.016.
Values are sent between devices in bfloat16 or wider.
A program may use at most 2 GiB of HBM per device.

```python
import jax
import jax.numpy as jnp

ROWS = 2048
D = 7168
FF = 20480


def setup_inputs(seed: int = 0, part: int = 0) -> dict:
    kx, kg, ku, kd = jax.random.split(jax.random.key(seed), 4)
    drawn = {
        "x": jax.random.normal(jax.random.fold_in(kx, part), (ROWS, D), jnp.float32),
        "w_gate": jax.random.normal(kg, (D, FF), jnp.float32) * D**-0.5,
        "w_up": jax.random.normal(ku, (D, FF), jnp.float32) * D**-0.5,
        "w_down": jax.random.normal(kd, (FF, D), jnp.float32) * FF**-0.5,
    }
    return {k: v.astype(jnp.bfloat16) for k, v in drawn.items()}


def reference(x, w_gate, w_up, w_down):
    gate = jnp.dot(x, w_gate, preferred_element_type=jnp.float32)
    up = jnp.dot(x, w_up, preferred_element_type=jnp.float32)
    hidden = (jax.nn.silu(gate) * up).astype(jnp.bfloat16)
    return jnp.dot(hidden, w_down, preferred_element_type=jnp.float32).astype(jnp.bfloat16)
```

```python
import jax
import jax.numpy as jnp
from jax import lax
from jax.sharding import PartitionSpec as P

CHUNKS = (256, 512, 640, 640)


def solution(mesh):
    def step(x, w_gate, w_up, w_down):
        outs = []
        start = 0
        for rows in CHUNKS:
            xs = x[start : start + rows]
            start += rows
            gate = jnp.dot(xs, w_gate, preferred_element_type=jnp.float32)
            up = jnp.dot(xs, w_up, preferred_element_type=jnp.float32)
            hidden = (jax.nn.silu(gate) * up).astype(jnp.bfloat16)
            term = jnp.dot(hidden, w_down, preferred_element_type=jnp.float32).astype(jnp.bfloat16)
            if outs:
                term, outs[-1] = lax.optimization_barrier((term, outs[-1]))
            outs.append(lax.psum(term, "tp"))
        return jnp.concatenate(outs, axis=0)

    return jax.shard_map(
        step,
        mesh=mesh,
        in_specs=(P("dp", None), P(None, "tp"), P(None, "tp"), P("tp", None)),
        out_specs=P("dp", None),
        check_vma=False,
    )
```

```python
import functools

import jax
import jax.numpy as jnp
from jax import lax
from jax.experimental import pallas as pl
from jax.experimental.pallas import tpu as pltpu
from jax.sharding import PartitionSpec as P

BF16 = jnp.bfloat16
F32 = jnp.float32
R = 512
GT = 256
W = 512
MESH = pl.DeviceIdType.MESH


def kernel(
    n_chunks, n_gu, n_u,
    x_hbm, wg_hbm, wu_hbm, wd_hbm, y_hbm,
    xbuf, hid, wgu, wdb, obuf, orecv, sbuf, r1, r2,
    x_sem, wgu_sem, wd_sem, o_ss, o_rs, r1_ss, r1_rs, r2_ss, r2_rs,
    a1_ss, a1_rs, a2_ss, a2_rs, a3_ss, a3_rs, loc_sem, d_ss, d_rs, credit,
):
    me = lax.axis_index("tp")
    dp = lax.axis_index("dp")
    c = lax.rem(me, 2)
    cy = lax.rem(me // 2, 2)
    cx = me // 4
    partner = me + 1 - 2 * c
    xn = me + 4 - 8 * cx
    yn = me + 2 - 4 * cy
    half = n_u * W
    n_dn = 2 * n_u
    q, h = R // 8, R // 4

    def dev(i):
        return (dp, i)

    def x_copy(i):
        return pltpu.make_async_copy(x_hbm.at[pl.ds(i * R, R), :], xbuf, x_sem)

    def gu_copies(g):
        slot = lax.rem(g, 2)
        col = pl.multiple_of(lax.rem(g, n_gu) * GT, GT)
        return [
            pltpu.make_async_copy(
                w.at[:, pl.ds(col, GT)], wgu.at[slot, :, pl.ds(k * GT, GT)], wgu_sem.at[slot, k]
            )
            for k, w in enumerate((wg_hbm, wu_hbm))
        ]

    def wd_copy(g):
        n = lax.rem(g, n_dn)
        slot = lax.rem(g, 3)
        odd = lax.rem(n, 2) == 1
        last = n == n_dn - 1
        own = jnp.logical_or(last, jnp.logical_and(jnp.logical_not(odd), n > 0))
        tile = jnp.where(last, n_u - 1, jnp.where(odd, (n + 1) // 2, jnp.maximum(n // 2 - 1, 0)))
        col = pl.multiple_of(jnp.where(own, c, 1 - c) * half + tile * W, W)
        return pltpu.make_async_copy(wd_hbm.at[:, pl.ds(col, W)], wdb.at[slot], wd_sem.at[slot])

    def remote(src, dst, ss, rs, to):
        return pltpu.make_async_remote_copy(
            src_ref=src, dst_ref=dst, send_sem=ss, recv_sem=rs, device_id=dev(to), device_id_type=MESH
        )

    def o_send(u):
        return remote(obuf.at[u], orecv.at[u], o_ss.at[u], o_rs.at[u], partner)

    first = (xn, yn)
    second = (yn, xn)
    f_bit = (cx, cy)
    s_bit = (cy, cx)

    def keep1(k):
        return pl.multiple_of(k * (R // 2) + f_bit[k] * h, h)

    def give1(k):
        return pl.multiple_of(k * (R // 2) + (1 - f_bit[k]) * h, h)

    def keep2(k):
        return pl.multiple_of(keep1(k) + s_bit[k] * q, q)

    def give2(k):
        return pl.multiple_of(keep1(k) + (1 - s_bit[k]) * q, q)

    def rs1(k, u):
        return remote(
            sbuf.at[u, pl.ds(give1(k), h), :], r1.at[k, u], r1_ss.at[k, u], r1_rs.at[k, u], first[k]
        )

    def rs2(k, u):
        return remote(
            sbuf.at[u, pl.ds(give2(k), q), :], r2.at[k, u], r2_ss.at[k, u], r2_rs.at[k, u], second[k]
        )

    def place(i, u, row, rows):
        col = pl.multiple_of(c * half + u * W, W)
        return y_hbm.at[pl.ds(pl.multiple_of(i * R + row, q), rows), pl.ds(col, W)]

    def ag1(k, i, u):
        return remote(
            sbuf.at[u, pl.ds(keep2(k), q), :], place(i, u, keep2(k), q),
            a1_ss.at[k, u], a1_rs.at[k, u], second[k],
        )

    def ag2(k, i, u):
        return remote(
            sbuf.at[u, pl.ds(keep2(k), q), :], place(i, u, keep2(k), q),
            a2_ss.at[k, u], a2_rs.at[k, u], first[k],
        )

    def ag3(k, i, u):
        at = place(i, u, give2(k), q)
        return remote(at, at, a3_ss.at[k, u], a3_rs.at[k, u], first[k])

    def local(k, i, u):
        return pltpu.make_async_copy(
            sbuf.at[u, pl.ds(keep2(k), q), :], place(i, u, keep2(k), q), loc_sem.at[k, u]
        )

    def across(i, u):
        at = place(i, u, 0, R)
        return remote(at, at, d_ss.at[i, u], d_rs.at[i, u], partner)

    def p1(i, u):
        for k in range(2):
            rs1(k, u).wait_recv()
            rows = pl.ds(keep1(k), h)
            sbuf[u, rows, :] = (sbuf[u, rows, :].astype(F32) + r1[k, u].astype(F32)).astype(BF16)
            rs2(k, u).start()

    def p2(i, u):
        for k in range(2):
            rs2(k, u).wait_recv()
            rows = pl.ds(keep2(k), q)
            sbuf[u, rows, :] = (sbuf[u, rows, :].astype(F32) + r2[k, u].astype(F32)).astype(BF16)
            ag1(k, i, u).start()
            ag2(k, i, u).start()
            local(k, i, u).start()

    def p3(i, u):
        for k in range(2):
            ag1(k, i, u).wait_recv()
            ag3(k, i, u).start()

    def p4(i, u):
        for k in range(2):
            ag2(k, i, u).wait_recv()
            ag3(k, i, u).wait_recv()
            local(k, i, u).wait()
            rs1(k, u).wait_send()
            rs2(k, u).wait_send()
            ag1(k, i, u).wait_send()
            ag2(k, i, u).wait_send()
            ag3(k, i, u).wait_send()
        across(i, u).start()

    def loop(lo, hi, f):
        def body(s, carry):
            f(s)
            return carry

        lax.fori_loop(lo, hi, body, 0)

    x_copy(0).start()
    for g in range(2):
        for cp in gu_copies(g):
            cp.start()
    for g in range(3):
        wd_copy(g).start()
    barrier = pltpu.get_barrier_semaphore()
    for other in (partner, xn, yn):
        pl.semaphore_signal(barrier, inc=1, device_id=dev(other), device_id_type=MESH)
    pl.semaphore_wait(barrier, 3)

    def chunk(i):
        x_copy(i).wait()
        prev = i - 1

        def gu(j):
            g = i * n_gu + j

            @pl.when(i > 0)
            def _():
                @pl.when(j == 0)
                def _():
                    loop(n_u - 2, n_u, lambda u: p1(prev, u))

                loop(jnp.minimum(2 * j, n_u), jnp.minimum(2 * j + 2, n_u), lambda u: p2(prev, u))
                b = 2 * jnp.maximum(j - 3, 0)
                t = 2 * jnp.maximum(j - 2, 0)
                loop(jnp.minimum(b, n_u), jnp.minimum(t, n_u), lambda u: p3(prev, u))

            slot = lax.rem(g, 2)
            for cp in gu_copies(g):
                cp.wait()
            r = jnp.dot(xbuf[...], wgu[slot], preferred_element_type=F32)
            gate, up = r[:, :GT], r[:, GT:]
            hid[:, pl.ds(pl.multiple_of(j * GT, GT), GT)] = (jax.nn.silu(gate) * up).astype(BF16)

            @pl.when(g + 2 < n_chunks * n_gu)
            def _():
                for cp in gu_copies(g + 2):
                    cp.start()

        loop(0, n_gu, gu)

        @pl.when(i + 1 < n_chunks)
        def _():
            x_copy(i + 1).start()

        def next_wd(g):
            @pl.when(g + 3 < n_chunks * n_dn)
            def _():
                wd_copy(g + 3).start()

        def down(k):
            @pl.when(k < n_u)
            def _():
                @pl.when(i > 0)
                def _():
                    o_send(k).wait_send()

                    @pl.when(k == 0)
                    def _():
                        pl.semaphore_wait(credit, 1)

                g = i * n_dn + jnp.maximum(2 * k - 1, 0)
                wd_copy(g).wait()
                r = jnp.dot(hid[...], wdb[lax.rem(g, 3)], preferred_element_type=F32)
                obuf[k] = r.astype(BF16)
                o_send(k).start()
                next_wd(g)

            @pl.when(k > 0)
            def _():
                u = k - 1

                @pl.when(i > 0)
                def _():
                    p4(prev, u)

                g = i * n_dn + jnp.minimum(2 * k, n_dn - 1)
                wd_copy(g).wait()
                o_send(u).wait_recv()
                r = jnp.dot(hid[...], wdb[lax.rem(g, 3)], preferred_element_type=F32)
                sbuf[u] = (r + orecv[u].astype(F32)).astype(BF16)
                for color in range(2):
                    rs1(color, u).start()
                next_wd(g)

            @pl.when(k > 2)
            def _():
                p1(i, k - 3)

        loop(0, n_u + 1, down)

        @pl.when(i + 1 < n_chunks)
        def _():
            pl.semaphore_signal(credit, inc=1, device_id=dev(partner), device_id_type=MESH)

    loop(0, n_chunks, chunk)

    end = n_chunks - 1
    loop(n_u - 2, n_u, lambda u: p1(end, u))

    def tail(s):
        @pl.when(s < n_u)
        def _():
            p2(end, s)

        @pl.when(jnp.logical_and(s >= 2, s < n_u + 2))
        def _():
            p3(end, s - 2)

        @pl.when(s >= 4)
        def _():
            p4(end, s - 4)

    loop(0, n_u + 4, tail)

    def drain(u):
        o_send(u).wait_send()

        def one(i):
            across(i, u).wait_send()
            across(i, u).wait_recv()

        loop(0, n_chunks, one)

    loop(0, n_u, drain)


def solution(mesh):
    def step(x, w_gate, w_up, w_down):
        rows, d = x.shape
        ff = w_gate.shape[1]
        n_chunks, n_gu, n_u = rows // R, ff // GT, d // (2 * W)
        dma = pltpu.SemaphoreType.DMA
        pair = (2, n_u)
        any_space = pl.BlockSpec(memory_space=pl.ANY)
        return pl.pallas_call(
            functools.partial(kernel, n_chunks, n_gu, n_u),
            out_shape=jax.ShapeDtypeStruct((rows, d), BF16),
            in_specs=[any_space] * 4,
            out_specs=any_space,
            scratch_shapes=[
                pltpu.VMEM((R, d), BF16),
                pltpu.VMEM((R, ff), BF16),
                pltpu.VMEM((2, d, 2 * GT), BF16),
                pltpu.VMEM((3, ff, W), BF16),
                pltpu.VMEM((n_u, R, W), BF16),
                pltpu.VMEM((n_u, R, W), BF16),
                pltpu.VMEM((n_u, R, W), BF16),
                pltpu.VMEM((2, n_u, R // 4, W), BF16),
                pltpu.VMEM((2, n_u, R // 8, W), BF16),
                dma, dma((2, 2)), dma((3,)),
                dma((n_u,)), dma((n_u,)),
                *[dma(pair) for _ in range(10)],
                dma(pair),
                dma((n_chunks, n_u)), dma((n_chunks, n_u)),
                pltpu.SemaphoreType.REGULAR,
            ],
            compiler_params=pltpu.CompilerParams(
                collective_id=0, has_side_effects=True, vmem_limit_bytes=62 * 1024 * 1024
            ),
            name="mlp_reduce",
        )(x, w_gate, w_up, w_down)

    return jax.shard_map(
        step,
        mesh=mesh,
        in_specs=(P("dp", None), P(None, "tp"), P(None, "tp"), P("tp", None)),
        out_specs=P("dp", None),
        check_vma=False,
    )
```

```python
import functools

import jax
import jax.numpy as jnp
from jax import lax
from jax.experimental import pallas as pl
from jax.experimental.pallas import tpu as pltpu
from jax.sharding import PartitionSpec as P

BF16 = jnp.bfloat16
F32 = jnp.float32
MAIN, LAST = 448, 256
GT = 256
W = 512
V = W // 2
SLOTS = 4
END_P1, END_P2 = 5, 8
D2, D3, D4 = 1, 3, 5
O_LEAD = 2
P1_LAG = 8
P2_AT, P3_AT, P3_EACH = 3, 8, 4
MESH = pl.DeviceIdType.MESH


def when(cond, f):
    if isinstance(cond, bool):
        if cond:
            f()
    else:
        pl.when(cond)(f)


def loop(lo, hi, f):
    def body(s, carry):
        f(s)
        return carry

    lax.fori_loop(lo, hi, body, 0)


def kernel(
    n_main, n_gu, n_u,
    x_hbm, wg_hbm, wu_hbm, wd_hbm, y_hbm,
    xbuf, hid, wgu, wdb, obuf, orecv, sbuf, r1, r2,
    x_sem, wgu_sem, wd_sem, o_ss, o_rs, r1_ss, r1_rs, r2_ss, r2_rs,
    a1_ss, a1_rs, a2_ss, a2_rs, a3_ss, a3_rs, loc_sem, d_ss, d_rs, credit,
):
    me = lax.axis_index("tp")
    dp = lax.axis_index("dp")
    c = lax.rem(me, 2)
    cy = lax.rem(me // 2, 2)
    cx = me // 4
    partner = me + 1 - 2 * c
    xn = me + 4 - 8 * cx
    yn = me + 2 - 4 * cy
    half = n_u * W
    n_dn = 2 * n_u
    n_chunks = n_main + 1

    def dev(i):
        return (dp, i)

    def size(i):
        return LAST if isinstance(i, int) and i == n_main else MAIN

    def x_copy(i):
        rows = size(i)
        at = pl.ds(pl.multiple_of(i * MAIN, MAIN), rows)
        slot = lax.rem(jnp.int32(i), 2)
        return pltpu.make_async_copy(x_hbm.at[at, :], xbuf.at[slot, pl.ds(0, rows), :], x_sem.at[slot])

    def gu_copies(g):
        slot = lax.rem(g, 2)
        col = pl.multiple_of(lax.rem(g, n_gu) * GT, GT)
        return [
            pltpu.make_async_copy(
                w.at[:, pl.ds(col, GT)], wgu.at[slot, :, pl.ds(k * GT, GT)], wgu_sem.at[slot, k]
            )
            for k, w in enumerate((wg_hbm, wu_hbm))
        ]

    def o_index(u):
        return jnp.maximum(2 * u - O_LEAD, jnp.minimum(u, O_LEAD))

    def w_index(u):
        return jnp.minimum(2 * u + O_LEAD + 1, n_u + u)

    def wd_copy(g):
        n = lax.rem(g, n_dn)
        slot = lax.rem(g, SLOTS)
        m = n - O_LEAD
        head, tail = n < O_LEAD, n >= n_dn - O_LEAD
        even = lax.rem(m + 2 * O_LEAD, 2) == 0
        own = jnp.logical_or(tail, jnp.logical_and(jnp.logical_not(head), jnp.logical_not(even)))
        mid = jnp.where(even, O_LEAD + m // 2, m // 2)
        tile = jnp.where(head, n, jnp.where(tail, n - n_u, mid))
        col = pl.multiple_of(jnp.where(own, c, 1 - c) * half + tile * W, W)
        return pltpu.make_async_copy(wd_hbm.at[:, pl.ds(col, W)], wdb.at[slot], wd_sem.at[slot])

    def remote(src, dst, ss, rs, to):
        return pltpu.make_async_remote_copy(
            src_ref=src, dst_ref=dst, send_sem=ss, recv_sem=rs, device_id=dev(to), device_id_type=MESH
        )

    def o_send(i, u):
        rows = pl.ds(0, size(i))
        return remote(obuf.at[u, rows, :], orecv.at[u, rows, :], o_ss.at[u], o_rs.at[u], partner)

    first = (xn, yn)
    second = (yn, xn)
    f_bit = (cx, cy)
    s_bit = (cy, cx)

    def keep1(i, k):
        h = size(i) // 2
        return pl.multiple_of(f_bit[k] * h, h)

    def give1(i, k):
        h = size(i) // 2
        return pl.multiple_of((1 - f_bit[k]) * h, h)

    def keep2(i, k):
        q = size(i) // 4
        return pl.multiple_of(keep1(i, k) + s_bit[k] * q, q)

    def give2(i, k):
        q = size(i) // 4
        return pl.multiple_of(keep1(i, k) + (1 - s_bit[k]) * q, q)

    def rs1(i, k, u):
        h = size(i) // 2
        return remote(
            sbuf.at[k, u, pl.ds(give1(i, k), h), :], r1.at[k, u, pl.ds(0, h), :],
            r1_ss.at[k, u], r1_rs.at[k, u], first[k],
        )

    def rs2(i, k, u):
        q = size(i) // 4
        return remote(
            sbuf.at[k, u, pl.ds(give2(i, k), q), :], r2.at[k, u, pl.ds(0, q), :],
            r2_ss.at[k, u], r2_rs.at[k, u], second[k],
        )

    def place(i, k, u, row):
        q = size(i) // 4
        col = pl.multiple_of(c * half + u * W + k * V, V)
        return y_hbm.at[pl.ds(pl.multiple_of(i * MAIN + row, q), q), pl.ds(col, V)]

    def piece(i, k, u):
        q = size(i) // 4
        return sbuf.at[k, u, pl.ds(keep2(i, k), q), :], place(i, k, u, keep2(i, k))

    def ag1(i, k, u):
        return remote(*piece(i, k, u), a1_ss.at[k, u], a1_rs.at[k, u], second[k])

    def ag2(i, k, u):
        return remote(*piece(i, k, u), a2_ss.at[k, u], a2_rs.at[k, u], first[k])

    def ag3(i, k, u):
        at = place(i, k, u, give2(i, k))
        return remote(at, at, a3_ss.at[k, u], a3_rs.at[k, u], first[k])

    def local(i, k, u):
        return pltpu.make_async_copy(*piece(i, k, u), loc_sem.at[k, u])

    def across(i, u):
        col = pl.multiple_of(c * half + u * W, W)
        at = y_hbm.at[pl.ds(pl.multiple_of(i * MAIN, MAIN), size(i)), pl.ds(col, W)]
        return remote(at, at, d_ss.at[i, u], d_rs.at[i, u], partner)

    def p1(i, u):
        h = size(i) // 2
        for k in range(2):
            rs1(i, k, u).wait_recv()
            rows = pl.ds(keep1(i, k), h)
            sbuf[k, u, rows, :] = (sbuf[k, u, rows, :].astype(F32) + r1[k, u, :h].astype(F32)).astype(BF16)
            rs2(i, k, u).start()

    def p2(i, u):
        q = size(i) // 4
        for k in range(2):
            rs2(i, k, u).wait_recv()
            rows = pl.ds(keep2(i, k), q)
            sbuf[k, u, rows, :] = (sbuf[k, u, rows, :].astype(F32) + r2[k, u, :q].astype(F32)).astype(BF16)
            ag1(i, k, u).start()
            ag2(i, k, u).start()
            local(i, k, u).start()

    def p3(i, u):
        for k in range(2):
            ag1(i, k, u).wait_recv()
            ag3(i, k, u).start()

    def p4(i, u):
        for k in range(2):
            ag2(i, k, u).wait_recv()
            ag3(i, k, u).wait_recv()
            local(i, k, u).wait()
            rs1(i, k, u).wait_send()
            rs2(i, k, u).wait_send()
            ag1(i, k, u).wait_send()
            ag2(i, k, u).wait_send()
            ag3(i, k, u).wait_send()
        across(i, u).start()

    p1_left = n_u + O_LEAD - P1_LAG

    x_copy(0).start()
    for g in range(2):
        for cp in gu_copies(g):
            cp.start()
    for g in range(SLOTS):
        wd_copy(g).start()
    barrier = pltpu.get_barrier_semaphore()
    for other in (partner, xn, yn):
        pl.semaphore_signal(barrier, inc=1, device_id=dev(other), device_id_type=MESH)
    pl.semaphore_wait(barrier, 3)

    def chunk(i):
        rows = size(i)
        final = isinstance(i, int)
        prev = i - 1 if not final else jnp.int32(i - 1)
        later = True if final else i > 0
        x_copy(i).wait()
        if not final:
            when(i + 1 < n_main, lambda: x_copy(i + 1).start())
            when(i + 1 == n_main, lambda: x_copy(n_main).start())
        xs = lax.rem(jnp.int32(i), 2)

        def gu(j):
            g = i * n_gu + j

            def reduce():
                def span(at, start, f, each=2):
                    lo = start + each * jnp.maximum(j - at, 0)
                    hi = start + each * jnp.maximum(j - at + 1, 0)
                    loop(jnp.minimum(lo, n_u), jnp.minimum(hi, n_u), lambda u: f(prev, u))

                span(0, p1_left, p1)
                span(P2_AT, 0, p2)
                span(P3_AT, 0, p3, P3_EACH)

            when(later, reduce)
            slot = lax.rem(g, 2)
            for cp in gu_copies(g):
                cp.wait()
            r = jnp.dot(xbuf[xs, :rows], wgu[slot], preferred_element_type=F32)
            gate, up = r[:, :GT], r[:, GT:]
            at = pl.ds(pl.multiple_of(j * GT, GT), GT)
            hid[:rows, at] = (jax.nn.silu(gate) * up).astype(BF16)

            def fetch():
                for cp in gu_copies(g + 2):
                    cp.start()

            when(g + 2 < n_chunks * n_gu, fetch)

        loop(0, n_gu, gu)

        def product(g):
            return jnp.dot(hid[:rows, :], wdb[lax.rem(g, SLOTS)], preferred_element_type=F32)

        def next_wd(g):
            when(g + SLOTS < n_chunks * n_dn, lambda: wd_copy(g + SLOTS).start())

        def down(t, other, own):
            k, u = t, t - O_LEAD
            g_k, g_u = i * n_dn + o_index(k), i * n_dn + w_index(u)
            if other:
                def reuse():
                    o_send(prev, k).wait_send()
                    when(k == 0, lambda: pl.semaphore_wait(credit, 1))

                when(later, reuse)
                wd_copy(g_k).wait()
            if own:
                when(later, lambda: p4(prev, u))
                wd_copy(g_u).wait()
                o_send(i, u).wait_recv()
            if other:
                obuf[k, :rows] = product(g_k).astype(BF16)
            if own:
                total = (product(g_u) + orecv[u, :rows].astype(F32)).astype(BF16)
                for k2 in range(2):
                    sbuf[k2, u, :rows] = total[:, k2 * V : (k2 + 1) * V]
            if other:
                o_send(i, k).start()
                next_wd(g_k)
            if own:
                for k2 in range(2):
                    rs1(i, k2, u).start()
                next_wd(g_u)
                if final:
                    when(t >= END_P1, lambda: p1(i, t - END_P1))
                    when(t >= END_P2, lambda: p2(i, t - END_P2))
                else:
                    when(t >= P1_LAG, lambda: p1(i, t - P1_LAG))

        loop(0, O_LEAD, lambda t: down(t, True, False))
        loop(O_LEAD, n_u, lambda t: down(t, True, True))
        loop(n_u, n_u + O_LEAD, lambda t: down(t, False, True))
        if not final:
            pl.semaphore_signal(credit, inc=1, device_id=dev(partner), device_id_type=MESH)

    loop(0, n_main, chunk)
    chunk(n_main)

    def tail(s):
        when(jnp.logical_and(s >= p1_end, s < n_u), lambda: p1(n_main, s))
        when(jnp.logical_and(s >= p2_end + D2, s < n_u + D2), lambda: p2(n_main, s - D2))
        when(jnp.logical_and(s >= D3, s < n_u + D3), lambda: p3(n_main, s - D3))
        when(s >= D4, lambda: p4(n_main, s - D4))

    p1_end, p2_end = n_u + O_LEAD - END_P1, max(n_u + O_LEAD - END_P2, 0)
    loop(min(p1_end, p2_end + D2, D3), n_u + D4, tail)

    def drain(u):
        o_send(n_main, u).wait_send()

        def one(i):
            across(i, u).wait_send()
            across(i, u).wait_recv()

        loop(0, n_main, one)
        one(n_main)

    loop(0, n_u, drain)


def solution(mesh):
    def step(x, w_gate, w_up, w_down):
        rows, d = x.shape
        ff = w_gate.shape[1]
        n_main, n_gu, n_u = (rows - LAST) // MAIN, ff // GT, d // (2 * W)
        dma = pltpu.SemaphoreType.DMA
        pair = (2, n_u)
        any_space = pl.BlockSpec(memory_space=pl.ANY)
        return pl.pallas_call(
            functools.partial(kernel, n_main, n_gu, n_u),
            out_shape=jax.ShapeDtypeStruct((rows, d), BF16),
            in_specs=[any_space] * 4,
            out_specs=any_space,
            scratch_shapes=[
                pltpu.VMEM((2, MAIN, d), BF16),
                pltpu.VMEM((MAIN, ff), BF16),
                pltpu.VMEM((2, d, 2 * GT), BF16),
                pltpu.VMEM((SLOTS, ff, W), BF16),
                pltpu.VMEM((n_u, MAIN, W), BF16),
                pltpu.VMEM((n_u, MAIN, W), BF16),
                pltpu.VMEM((2, n_u, MAIN, V), BF16),
                pltpu.VMEM((2, n_u, MAIN // 2, V), BF16),
                pltpu.VMEM((2, n_u, MAIN // 4, V), BF16),
                dma((2,)), dma((2, 2)), dma((SLOTS,)),
                dma((n_u,)), dma((n_u,)),
                *[dma(pair) for _ in range(10)],
                dma(pair),
                dma((n_main + 1, n_u)), dma((n_main + 1, n_u)),
                pltpu.SemaphoreType.REGULAR,
            ],
            compiler_params=pltpu.CompilerParams(
                collective_id=0, has_side_effects=True, vmem_limit_bytes=62 * 1024 * 1024
            ),
            name="mlp_reduce",
        )(x, w_gate, w_up, w_down)

    return jax.shard_map(
        step,
        mesh=mesh,
        in_specs=(P("dp", None), P(None, "tp"), P(None, "tp"), P("tp", None)),
        out_specs=P("dp", None),
        check_vma=False,
    )
```

```python
import functools

import jax
import jax.numpy as jnp
from jax import lax
from jax.experimental import pallas as pl
from jax.experimental.pallas import tpu as pltpu
from jax.sharding import PartitionSpec as P

BF16 = jnp.bfloat16
F32 = jnp.float32
MAIN, LAST = 448, 256
GT = 256
W = 512
V = W // 2
SLOTS = 4
END_P1, END_P2 = 5, 8
D2, D3, D4 = 1, 3, 5
O_LEAD = 2
P1_LAG = 8
P2_AT, P3_AT, P3_EACH = 3, 9, 7
MESH = pl.DeviceIdType.MESH


def when(cond, f):
    if isinstance(cond, bool):
        if cond:
            f()
    else:
        pl.when(cond)(f)


def loop(lo, hi, f):
    def body(s, carry):
        f(s)
        return carry

    lax.fori_loop(lo, hi, body, 0)


def kernel(
    n_main, n_gu, n_u,
    x_hbm, wg_hbm, wu_hbm, wd_hbm, y_hbm,
    xbuf, hid, wgu, wdb, obuf, orecv, sbuf, r1, r2,
    x_sem, wgu_sem, wd_sem, o_ss, o_rs, r1_ss, r1_rs, r2_ss, r2_rs,
    a1_ss, a1_rs, a2_ss, a2_rs, a3_ss, a3_rs, loc_sem, d_ss, d_rs, credit,
):
    me = lax.axis_index("tp")
    dp = lax.axis_index("dp")
    c = lax.rem(me, 2)
    cy = lax.rem(me // 2, 2)
    cx = me // 4
    partner = me + 1 - 2 * c
    xn = me + 4 - 8 * cx
    yn = me + 2 - 4 * cy
    half = n_u * W
    n_dn = 2 * n_u
    n_chunks = n_main + 1

    def dev(i):
        return (dp, i)

    def size(i):
        return LAST if isinstance(i, int) and i == n_main else MAIN

    def x_copy(i):
        rows = size(i)
        at = pl.ds(pl.multiple_of(i * MAIN, MAIN), rows)
        slot = lax.rem(jnp.int32(i), 2)
        return pltpu.make_async_copy(x_hbm.at[at, :], xbuf.at[slot, pl.ds(0, rows), :], x_sem.at[slot])

    def gu_copies(g):
        slot = lax.rem(g, 2)
        col = pl.multiple_of(lax.rem(g, n_gu) * GT, GT)
        return [
            pltpu.make_async_copy(
                w.at[:, pl.ds(col, GT)], wgu.at[slot, :, pl.ds(k * GT, GT)], wgu_sem.at[slot, k]
            )
            for k, w in enumerate((wg_hbm, wu_hbm))
        ]

    def o_index(u):
        return jnp.maximum(2 * u - O_LEAD, jnp.minimum(u, O_LEAD))

    def w_index(u):
        return jnp.minimum(2 * u + O_LEAD + 1, n_u + u)

    def wd_copy(g):
        n = lax.rem(g, n_dn)
        slot = lax.rem(g, SLOTS)
        m = n - O_LEAD
        head, tail = n < O_LEAD, n >= n_dn - O_LEAD
        even = lax.rem(m + 2 * O_LEAD, 2) == 0
        own = jnp.logical_or(tail, jnp.logical_and(jnp.logical_not(head), jnp.logical_not(even)))
        mid = jnp.where(even, O_LEAD + m // 2, m // 2)
        tile = jnp.where(head, n, jnp.where(tail, n - n_u, mid))
        col = pl.multiple_of(jnp.where(own, c, 1 - c) * half + tile * W, W)
        return pltpu.make_async_copy(wd_hbm.at[:, pl.ds(col, W)], wdb.at[slot], wd_sem.at[slot])

    def remote(src, dst, ss, rs, to):
        return pltpu.make_async_remote_copy(
            src_ref=src, dst_ref=dst, send_sem=ss, recv_sem=rs, device_id=dev(to), device_id_type=MESH
        )

    def o_send(i, u):
        rows = pl.ds(0, size(i))
        return remote(obuf.at[u, rows, :], orecv.at[u, rows, :], o_ss.at[u], o_rs.at[u], partner)

    first = (xn, yn)
    second = (yn, xn)
    f_bit = (cx, cy)
    s_bit = (cy, cx)

    def keep1(i, k):
        h = size(i) // 2
        return pl.multiple_of(f_bit[k] * h, h)

    def give1(i, k):
        h = size(i) // 2
        return pl.multiple_of((1 - f_bit[k]) * h, h)

    def keep2(i, k):
        q = size(i) // 4
        return pl.multiple_of(keep1(i, k) + s_bit[k] * q, q)

    def give2(i, k):
        q = size(i) // 4
        return pl.multiple_of(keep1(i, k) + (1 - s_bit[k]) * q, q)

    def rs1(i, k, u):
        h = size(i) // 2
        return remote(
            sbuf.at[k, u, pl.ds(give1(i, k), h), :], r1.at[k, u, pl.ds(0, h), :],
            r1_ss.at[k, u], r1_rs.at[k, u], first[k],
        )

    def rs2(i, k, u):
        q = size(i) // 4
        return remote(
            sbuf.at[k, u, pl.ds(give2(i, k), q), :], r2.at[k, u, pl.ds(0, q), :],
            r2_ss.at[k, u], r2_rs.at[k, u], second[k],
        )

    def place(i, k, u, row):
        q = size(i) // 4
        col = pl.multiple_of(c * half + u * W + k * V, V)
        return y_hbm.at[pl.ds(pl.multiple_of(i * MAIN + row, q), q), pl.ds(col, V)]

    def piece(i, k, u):
        q = size(i) // 4
        return sbuf.at[k, u, pl.ds(keep2(i, k), q), :], place(i, k, u, keep2(i, k))

    def ag1(i, k, u):
        return remote(*piece(i, k, u), a1_ss.at[k, u], a1_rs.at[k, u], second[k])

    def ag2(i, k, u):
        return remote(*piece(i, k, u), a2_ss.at[k, u], a2_rs.at[k, u], first[k])

    def ag3(i, k, u):
        at = place(i, k, u, give2(i, k))
        return remote(at, at, a3_ss.at[k, u], a3_rs.at[k, u], first[k])

    def local(i, k, u):
        return pltpu.make_async_copy(*piece(i, k, u), loc_sem.at[k, u])

    def across(i, u):
        col = pl.multiple_of(c * half + u * W, W)
        at = y_hbm.at[pl.ds(pl.multiple_of(i * MAIN, MAIN), size(i)), pl.ds(col, W)]
        return remote(at, at, d_ss.at[i, u], d_rs.at[i, u], partner)

    def p1(i, u):
        h = size(i) // 2
        for k in range(2):
            rs1(i, k, u).wait_recv()
            rows = pl.ds(keep1(i, k), h)
            sbuf[k, u, rows, :] = (sbuf[k, u, rows, :].astype(F32) + r1[k, u, :h].astype(F32)).astype(BF16)
            rs2(i, k, u).start()

    def p2(i, u):
        q = size(i) // 4
        for k in range(2):
            rs2(i, k, u).wait_recv()
            rows = pl.ds(keep2(i, k), q)
            sbuf[k, u, rows, :] = (sbuf[k, u, rows, :].astype(F32) + r2[k, u, :q].astype(F32)).astype(BF16)
            ag1(i, k, u).start()
        for k in range(2):
            ag2(i, k, u).start()
            local(i, k, u).start()

    def p3(i, u):
        for k in range(2):
            ag1(i, k, u).wait_recv()
            ag3(i, k, u).start()

    def p4(i, u):
        for k in range(2):
            ag2(i, k, u).wait_recv()
            ag3(i, k, u).wait_recv()
            local(i, k, u).wait()
            rs1(i, k, u).wait_send()
            rs2(i, k, u).wait_send()
            ag1(i, k, u).wait_send()
            ag2(i, k, u).wait_send()
            ag3(i, k, u).wait_send()
        across(i, u).start()

    p1_left = n_u + O_LEAD - P1_LAG

    x_copy(0).start()
    for cp in gu_copies(0):
        cp.start()
    barrier = pltpu.get_barrier_semaphore()
    for other in (partner, xn, yn):
        pl.semaphore_signal(barrier, inc=1, device_id=dev(other), device_id_type=MESH)
    pl.semaphore_wait(barrier, 3)

    def chunk(i):
        rows = size(i)
        final = isinstance(i, int)
        prev = i - 1 if not final else jnp.int32(i - 1)
        later = True if final else i > 0
        x_copy(i).wait()
        xs = lax.rem(jnp.int32(i), 2)

        def gu(j):
            g = i * n_gu + j

            def reduce():
                def span(at, start, f, each=2):
                    lo = start + each * jnp.maximum(j - at, 0)
                    hi = start + each * jnp.maximum(j - at + 1, 0)
                    loop(jnp.minimum(lo, n_u), jnp.minimum(hi, n_u), lambda u: f(prev, u))

                span(0, p1_left, p1)
                span(P2_AT, 0, p2)
                span(P3_AT, 0, p3, P3_EACH)

            when(later, reduce)
            slot = lax.rem(g, 2)
            for cp in gu_copies(g):
                cp.wait()
            if not final:
                def second():
                    for cp in gu_copies(1):
                        cp.start()

                def downs():
                    for n in range(SLOTS):
                        wd_copy(n).start()

                when(g == 0, second)
                when(g == 3, downs)
                when(jnp.logical_and(j == 5, i + 1 < n_main), lambda: x_copy(i + 1).start())
                when(jnp.logical_and(j == 5, i + 1 == n_main), lambda: x_copy(n_main).start())
            r = jnp.dot(xbuf[xs, :rows], wgu[slot], preferred_element_type=F32)
            gate, up = r[:, :GT], r[:, GT:]
            at = pl.ds(pl.multiple_of(j * GT, GT), GT)
            hid[:rows, at] = (jax.nn.silu(gate) * up).astype(BF16)

            def fetch():
                for cp in gu_copies(g + 2):
                    cp.start()

            when(g + 2 < n_chunks * n_gu, fetch)

        loop(0, n_gu, gu)

        def product(g):
            return jnp.dot(hid[:rows, :], wdb[lax.rem(g, SLOTS)], preferred_element_type=F32)

        def next_wd(g):
            when(g + SLOTS < n_chunks * n_dn, lambda: wd_copy(g + SLOTS).start())

        def down(t, other, own):
            k, u = t, t - O_LEAD
            g_k, g_u = i * n_dn + o_index(k), i * n_dn + w_index(u)
            if other:
                def reuse():
                    o_send(prev, k).wait_send()
                    when(k == 0, lambda: pl.semaphore_wait(credit, 1))

                when(later, reuse)
                wd_copy(g_k).wait()
            if own:
                when(later, lambda: p4(prev, u))
                wd_copy(g_u).wait()
                o_send(i, u).wait_recv()
            if other:
                obuf[k, :rows] = product(g_k).astype(BF16)
            if own:
                total = (product(g_u) + orecv[u, :rows].astype(F32)).astype(BF16)
                for k2 in range(2):
                    sbuf[k2, u, :rows] = total[:, k2 * V : (k2 + 1) * V]
            if other:
                o_send(i, k).start()
                next_wd(g_k)
            if own:
                for k2 in range(2):
                    rs1(i, k2, u).start()
                next_wd(g_u)
                if final:
                    when(t >= END_P1, lambda: p1(i, t - END_P1))
                    when(t >= END_P2, lambda: p2(i, t - END_P2))
                else:
                    when(t >= P1_LAG, lambda: p1(i, t - P1_LAG))

        loop(0, O_LEAD, lambda t: down(t, True, False))
        loop(O_LEAD, n_u, lambda t: down(t, True, True))
        loop(n_u, n_u + O_LEAD, lambda t: down(t, False, True))
        if not final:
            pl.semaphore_signal(credit, inc=1, device_id=dev(partner), device_id_type=MESH)

    loop(0, n_main, chunk)
    chunk(n_main)

    def tail(s):
        when(jnp.logical_and(s >= p1_end, s < n_u), lambda: p1(n_main, s))
        when(jnp.logical_and(s >= p2_end + D2, s < n_u + D2), lambda: p2(n_main, s - D2))
        when(jnp.logical_and(s >= D3, s < n_u + D3), lambda: p3(n_main, s - D3))
        when(s >= D4, lambda: p4(n_main, s - D4))

    p1_end, p2_end = n_u + O_LEAD - END_P1, max(n_u + O_LEAD - END_P2, 0)
    loop(min(p1_end, p2_end + D2, D3), n_u + D4, tail)

    def drain(u):
        o_send(n_main, u).wait_send()

        def one(i):
            across(i, u).wait_send()
            across(i, u).wait_recv()

        loop(0, n_main, one)
        one(n_main)

    loop(0, n_u, drain)


def solution(mesh):
    def step(x, w_gate, w_up, w_down):
        rows, d = x.shape
        ff = w_gate.shape[1]
        n_main, n_gu, n_u = (rows - LAST) // MAIN, ff // GT, d // (2 * W)
        dma = pltpu.SemaphoreType.DMA
        pair = (2, n_u)
        any_space = pl.BlockSpec(memory_space=pl.ANY)
        return pl.pallas_call(
            functools.partial(kernel, n_main, n_gu, n_u),
            out_shape=jax.ShapeDtypeStruct((rows, d), BF16),
            in_specs=[any_space] * 4,
            out_specs=any_space,
            scratch_shapes=[
                pltpu.VMEM((2, MAIN, d), BF16),
                pltpu.VMEM((MAIN, ff), BF16),
                pltpu.VMEM((2, d, 2 * GT), BF16),
                pltpu.VMEM((SLOTS, ff, W), BF16),
                pltpu.VMEM((n_u, MAIN, W), BF16),
                pltpu.VMEM((n_u, MAIN, W), BF16),
                pltpu.VMEM((2, n_u, MAIN, V), BF16),
                pltpu.VMEM((2, n_u, MAIN // 2, V), BF16),
                pltpu.VMEM((2, n_u, MAIN // 4, V), BF16),
                dma((2,)), dma((2, 2)), dma((SLOTS,)),
                dma((n_u,)), dma((n_u,)),
                *[dma(pair) for _ in range(10)],
                dma(pair),
                dma((n_main + 1, n_u)), dma((n_main + 1, n_u)),
                pltpu.SemaphoreType.REGULAR,
            ],
            compiler_params=pltpu.CompilerParams(
                collective_id=0, has_side_effects=True, vmem_limit_bytes=62 * 1024 * 1024
            ),
            name="mlp_reduce",
        )(x, w_gate, w_up, w_down)

    return jax.shard_map(
        step,
        mesh=mesh,
        in_specs=(P("dp", None), P(None, "tp"), P(None, "tp"), P("tp", None)),
        out_specs=P("dp", None),
        check_vma=False,
    )
```
